32 devices in a mesh: shard: 2 (over core), model: 4 (over y, x), unit: 4 (over z).
Axes of the slice: x: 2, y: 2, z: 4, core: 2. Of those that a mesh axis runs over, the one named last changes fastest.
Arguments:
- train_query: bfloat16 [16384, 4096], P(('unit', 'shard'), 'model'), parts along dimension 0, may hold values from -0.125 to 0.125
- low_query: bfloat16 [16384, 16], P(('unit', 'shard')), parts along dimension 0, may hold values from -0.09375 to 0.09375
- high_query: bfloat16 [64, 4096], P('unit', 'model'), parts along dimension 0, may hold values from -1.5 to 1.5
- train_key: bfloat16 [16384, 1024], P(('unit', 'shard'), 'model'), parts along dimension 0, may hold values from -0.125 to 0.125
- low_key: bfloat16 [16384, 16], P(('unit', 'shard')), parts along dimension 0, may hold values from -0.09375 to 0.09375
- high_key: bfloat16 [64, 1024], P('unit', 'model'), parts along dimension 0, may hold values from -1.5 to 1.5
- train_value: bfloat16 [16384, 1024], P(('unit', 'shard'), 'model'), parts along dimension 0, may hold values from -0.125 to 0.125
- low_value: bfloat16 [16384, 16], P(('unit', 'shard')), parts along dimension 0, may hold values from -0.09375 to 0.09375
- high_value: bfloat16 [64, 1024], P('unit', 'model'), parts along dimension 0, may hold values from -1.5 to 1.5
- norm_train: float32 [16384], P(('unit', 'shard', 'model')), parts along dimension 0, may hold values from 0.25 to 1.75
- norm_step: float32 [16384], P(('unit', 'shard', 'model')), parts along dimension 0, may hold values from -0.3 to 0.3
Outputs:
- serving_query: bfloat16 [16384, 4096], P('unit', 'model'), parts along dimension 0
- serving_key: bfloat16 [16384, 1024], P('unit', 'model'), parts along dimension 0
- serving_value: bfloat16 [16384, 1024], P('unit', 'model'), parts along dimension 0
- scale_query: float32 [16384], P(('unit', 'model')), parts along dimension 0
- scale_key: float32 [4096], P(('unit', 'model')), parts along dimension 0
- scale_value: float32 [4096], P(('unit', 'model')), parts along dimension 0
- serve_norm: bfloat16 [16384], P('unit'), parts along dimension 0
The draws below stay inside these ranges and needn't reach their ends.
There are 4 independent parts, one for each index of `unit`. The reference program is written for one: setup_inputs(seed, part) draws one part's arguments, and reference() takes and returns one part's arrays. A program takes and returns all parts, laid end to end along the dimension named above; each array names one. Nothing has to cross between parts.
All inputs are finite; a program needn't handle non-finite values. Where the reference program divides by a largest or mean magnitude, that divisor is 1e-20 or more.
Results may differ from the reference program's by a relative error of at most 0.001.
Values may be sent and summed in bfloat16 or wider, within the bound.
A program may use at most 64 MiB of HBM per device.

```python
import jax
import jax.numpy as jnp

D_MODEL = 4096
Q_DIM = 4096
KV_DIM = 1024
RANK = 16


def with_spikes(values, key, source, target, shards_of, factor):
    owner, partner = [(jnp.arange(values.shape[position]) // (values.shape[position] // shards_of)).reshape([-1 if axis == position else 1 for axis in range(values.ndim)]) for position in (source, target)]
    chosen = jax.random.permutation(key, shards_of)[partner]
    strong = (owner == chosen) | (owner == (partner + shards_of // 2) % shards_of)
    return jnp.where(strong, factor * values, values)


def block_levels(rng, extent, pieces, low, largest):
    loudness, own = 1.0, jax.random.fold_in(rng, 6)
    for dim, parts in pieces:
        steps = jnp.exp(jax.random.uniform(jax.random.fold_in(own, dim), (parts,), jnp.float32, low / len(pieces), largest / len(pieces)))
        loudness = loudness * jnp.repeat(steps, extent[dim] // parts).reshape([-1 if axis == dim else 1 for axis in range(len(extent))])
    return loudness


def bell_draw(key, dims, deviation, most, pieces=(), held_as=jnp.bfloat16):
    loudness = block_levels(key, dims, pieces, -0.22, 0.18) if pieces else 1.0
    drawn = jax.random.normal(key, dims, jnp.float32) * deviation * loudness
    return jnp.minimum(jnp.maximum(drawn, -most), most).astype(held_as)


def noise_with(rng, extent, width, most, shards, heavy, held_as=jnp.bfloat16):
    drawn = width * jax.random.normal(rng, extent, jnp.float32)
    if shards:
        drawn = drawn * block_levels(rng, extent, shards, -0.22, 0.18)
    return jnp.clip(with_spikes(drawn, jax.random.fold_in(rng, 3), *heavy), -most, most).astype(held_as)


def setup_inputs(seed: int = 0, part: int = 0) -> dict:
    key_list = jax.random.split(jax.random.key(seed), 12)
    part_splits = jax.random.split(jax.random.fold_in(key_list[11], part), 12)
    return {
        "train_query": noise_with(part_splits[0], (D_MODEL, Q_DIM), D_MODEL ** -0.5, 0.125, ((0, 2), (1, 4)), (0, 1, 4, 2.0)),
        "low_query": bell_draw(part_splits[1], (D_MODEL, RANK), D_MODEL ** -0.5, 0.09375, ((0, 2),)),
        "high_query": bell_draw(part_splits[2], (RANK, Q_DIM), RANK ** -0.5, 1.5, ((1, 4),)),
        "train_key": noise_with(part_splits[3], (D_MODEL, KV_DIM), D_MODEL ** -0.5, 0.125, ((0, 2), (1, 4)), (0, 1, 4, 2.0)),
        "low_key": bell_draw(part_splits[4], (D_MODEL, RANK), D_MODEL ** -0.5, 0.09375, ((0, 2),)),
        "high_key": bell_draw(part_splits[5], (RANK, KV_DIM), RANK ** -0.5, 1.5, ((1, 4),)),
        "train_value": noise_with(part_splits[6], (D_MODEL, KV_DIM), D_MODEL ** -0.5, 0.125, ((0, 2), (1, 4)), (0, 1, 4, 2.0)),
        "low_value": bell_draw(part_splits[7], (D_MODEL, RANK), D_MODEL ** -0.5, 0.09375, ((0, 2),)),
        "high_value": bell_draw(part_splits[8], (RANK, KV_DIM), RANK ** -0.5, 1.5, ((1, 4),)),
        "norm_train": jnp.clip(1.0 + 0.15 * jax.random.normal(part_splits[9], (D_MODEL,), jnp.float32), 0.25, 1.75),
        "norm_step": jnp.clip(jax.random.uniform(part_splits[10], (D_MODEL,), jnp.float32, -0.3, 0.3) * block_levels(part_splits[10], (D_MODEL,), ((0, 8),), -0.4, 0.0), -0.3, 0.3),
    }


mix_rate = 1.0


def reference(train_query, low_query, high_query, train_key, low_key, high_key, train_value, low_value, high_value, norm_train, norm_step):
    whole_query = train_query.astype(jnp.float32) + mix_rate * jnp.dot(low_query, high_query, preferred_element_type=jnp.float32)
    whole_key = train_key.astype(jnp.float32) + mix_rate * jnp.dot(low_key, high_key, preferred_element_type=jnp.float32)
    whole_value = train_value.astype(jnp.float32) + mix_rate * jnp.dot(low_value, high_value, preferred_element_type=jnp.float32)
    scale_query = jnp.max(jnp.abs(whole_query), axis=0)
    serving_query = (whole_query / scale_query).astype(jnp.bfloat16)
    scale_key = jnp.max(jnp.abs(whole_key), axis=0)
    serving_key = (whole_key / scale_key).astype(jnp.bfloat16)
    scale_value = jnp.max(jnp.abs(whole_value), axis=0)
    serving_value = (whole_value / scale_value).astype(jnp.bfloat16)
    serve_norm = (norm_train + norm_step).astype(jnp.bfloat16)
    return serving_query, serving_key, serving_value, scale_query, scale_key, scale_value, serve_norm
```

```python
import functools

import jax
import jax.numpy as jnp
from jax import lax
from jax.experimental import pallas as pl
from jax.experimental.pallas import tpu as pltpu
from jax.sharding import PartitionSpec as P

mix_rate = 1.0
MESH = pl.DeviceIdType.MESH
MIB = 1 << 20


def exchange_kernel(
    n_shard,
    n_model,
    chunks,
    tile,
    tq, lq, hq, tk, lk, hk, tv, lv, hv, nt, ns,
    wq, wk, wv, sq, sk, sv, norm,
    base, low_q, low_k, low_v, high_q, high_k, high_v, norms,
    send_base, recv_base, send_low, recv_low, local_high, send_norm, recv_norm,
):
    trains, lows, highs = (tq, tk, tv), (lq, lk, lv), (hq, hk, hv)
    low_bufs, high_bufs = (low_q, low_k, low_v), (high_q, high_k, high_v)
    wholes, scales = (wq, wk, wv), (sq, sk, sv)
    rows = tq.shape[0]
    shard, model = lax.axis_index("shard"), lax.axis_index("model")
    group = n_shard * n_model
    place = shard * n_model + model

    local = []
    for i in (1, 2, 0):
        local.append(pltpu.make_async_copy(lows[i], low_bufs[i].at[0], recv_low.at[0, i]))
        local.append(pltpu.make_async_copy(highs[i], high_bufs[i], local_high.at[i]))
    for c, (i, start, width) in enumerate(chunks):
        local.append(
            pltpu.make_async_copy(
                trains[i].at[:, pl.ds(start, width)], base.at[0, c], recv_base.at[0, c]
            )
        )
    local.append(pltpu.make_async_copy(nt, norms.at[place, 0], recv_norm.at[0, 0]))
    local.append(pltpu.make_async_copy(ns, norms.at[place, 1], recv_norm.at[0, 1]))

    barrier = pltpu.get_barrier_semaphore()
    for k in range(1, group):
        other = lax.rem(place + k, group)
        pl.semaphore_signal(
            barrier, inc=1,
            device_id={"shard": other // n_model, "model": lax.rem(other, n_model)},
            device_id_type=MESH,
        )
    for copy in local:
        copy.start()
    pl.semaphore_wait(barrier, group - 1)

    sends_low, sends_base, sends_norm = {}, {}, {}
    for d in range(1, n_shard):
        to = {"shard": lax.rem(shard + d, n_shard)}
        for i in (1, 2, 0):
            sends_low[d, i] = pltpu.make_async_remote_copy(
                src_ref=lows[i], dst_ref=low_bufs[i].at[d],
                send_sem=send_low.at[d, i], recv_sem=recv_low.at[d, i],
                device_id=to, device_id_type=MESH,
            )
            sends_low[d, i].start()
    for c, (i, start, width) in enumerate(chunks):
        for d in range(1, n_shard):
            to = {"shard": lax.rem(shard + d, n_shard)}
            sends_base[d, c] = pltpu.make_async_remote_copy(
                src_ref=trains[i].at[:, pl.ds(start, width)], dst_ref=base.at[d, c],
                send_sem=send_base.at[d, c], recv_sem=recv_base.at[d, c],
                device_id=to, device_id_type=MESH,
            )
            sends_base[d, c].start()
    for k in range(1, group):
        other = lax.rem(place + k, group)
        to = {"shard": other // n_model, "model": lax.rem(other, n_model)}
        for j, source in enumerate((nt, ns)):
            sends_norm[k, j] = pltpu.make_async_remote_copy(
                src_ref=source, dst_ref=norms.at[place, j],
                send_sem=send_norm.at[k, j], recv_sem=recv_norm.at[k, j],
                device_id=to, device_id_type=MESH,
            )
            sends_norm[k, j].start()

    for copy in local:
        copy.wait()

    def merge(d, c):
        i, start, width = chunks[c]
        first = lax.rem(shard - d + n_shard, n_shard) * rows
        high = high_bufs[i][:, start:start + width]

        def step(t, top):
            at = pl.multiple_of(t * tile, tile)
            product = lax.dot_general(
                low_bufs[i][d, :, pl.ds(at, tile)], high,
                (((0,), (0,)), ((), ())), preferred_element_type=jnp.float32,
            )
            whole = base[d, c, pl.ds(at, tile), :].astype(jnp.float32) + mix_rate * product
            wholes[i][pl.ds(pl.multiple_of(first + at, tile), tile), start:start + width] = whole
            return jnp.maximum(top, jnp.max(jnp.abs(whole).reshape(tile // 8, 8, width), axis=0))

        return lax.fori_loop(0, rows // tile, step, jnp.zeros((8, width), jnp.float32))

    tops = [merge(0, c) for c in range(len(chunks))]
    for d in range(1, n_shard):
        for i in (1, 2, 0):
            sends_low[d, i].wait()
    for c, (i, start, width) in enumerate(chunks):
        for d in range(1, n_shard):
            sends_base[d, c].wait()
            tops[c] = jnp.maximum(tops[c], merge(d, c))
        scales[i][:, start:start + width] = jnp.max(tops[c], axis=0, keepdims=True)
    for k in range(1, group):
        for j in range(2):
            sends_norm[k, j].wait()
    norm[...] = (norms[:, 0] + norms[:, 1]).reshape(norm.shape).astype(norm.dtype)


def scale_kernel(
    plan,
    wq, wk, wv, sq, sk, sv, norm,
    oq, ok, ov, osq, osk, osv, onorm,
    buf_q, buf_k, buf_v, sems,
):
    wholes, scales = (wq, wk, wv), (sq, sk, sv)
    outs, bufs = (oq, ok, ov), (buf_q, buf_k, buf_v)
    for source, target in ((sq, osq), (sk, osk), (sv, osv), (norm, onorm)):
        target[...] = source[...]
    for i, step, count, base in plan:
        inverse = 1.0 / scales[i][...]

        def copy(t):
            at = pl.multiple_of(t * step, step)
            return pltpu.make_async_copy(
                bufs[i].at[pl.ds(at, step), :], outs[i].at[pl.ds(at, step), :], sems.at[base + t]
            )

        @pl.loop(0, count)
        def _(t):
            at = pl.multiple_of(t * step, step)
            bufs[i][pl.ds(at, step), :] = (wholes[i][pl.ds(at, step), :] * inverse).astype(bufs[i].dtype)
            copy(t).start()

    for i, step, count, base in plan:
        @pl.loop(0, count)
        def _(t):
            at = pl.multiple_of(t * step, step)
            pltpu.make_async_copy(
                bufs[i].at[pl.ds(at, step), :], outs[i].at[pl.ds(at, step), :], sems.at[base + t]
            ).wait()


def local(n_shard, n_model, tq, lq, hq, tk, lk, hk, tv, lv, hv, nt, ns):
    rows, rank = tq.shape[0], hq.shape[0]
    widths = (tq.shape[1], tk.shape[1], tv.shape[1])
    width = min(min(widths), 256)
    tile = min(rows, 256)
    chunks = tuple((i, s, width) for i in (1, 2, 0) for s in range(0, widths[i], width))
    group = n_shard * n_model
    lanes = 128 if nt.shape[0] % 128 == 0 else nt.shape[0]
    piece = (nt.shape[0] // lanes, lanes)
    full = n_shard * rows
    f32, bf16 = jnp.float32, jnp.bfloat16
    dma = pltpu.SemaphoreType.DMA
    hbm, vmem = pl.BlockSpec(memory_space=pltpu.HBM), pl.BlockSpec(memory_space=pltpu.VMEM)
    norm_shape = (group * piece[0], lanes)

    parts = pl.pallas_call(
        functools.partial(exchange_kernel, n_shard, n_model, chunks, tile),
        out_shape=[pltpu.VMEM((full, w), f32) for w in widths]
        + [pltpu.VMEM((1, w), f32) for w in widths]
        + [pltpu.VMEM(norm_shape, bf16)],
        in_specs=[hbm] * 11,
        out_specs=[vmem] * 7,
        scratch_shapes=[pltpu.VMEM((n_shard, len(chunks), rows, width), bf16)]
        + [pltpu.VMEM((n_shard, rank, rows), bf16)] * 3
        + [pltpu.VMEM((rank, w), bf16) for w in widths]
        + [
            pltpu.VMEM((group, 2) + piece, f32),
            dma((n_shard, len(chunks))), dma((n_shard, len(chunks))),
            dma((n_shard, 3)), dma((n_shard, 3)), dma((3,)),
            dma((group, 2)), dma((group, 2)),
        ],
        compiler_params=pltpu.CompilerParams(
            collective_id=0, has_side_effects=True, vmem_limit_bytes=18 * MIB
        ),
        cost_estimate=pl.CostEstimate(flops=0, bytes_accessed=40 * MIB, transcendentals=0),
        name="exchange",
    )(*(pltpu.with_memory_space_constraint(x, pltpu.HBM) for x in (tq, lq.T, hq, tk, lk.T, hk, tv, lv.T, hv, nt.reshape(piece), ns.reshape(piece))))

    plan, base = [], 0
    for i in (0, 1, 2):
        step = min(full, 256 * max(widths) // widths[i])
        plan.append((i, step, full // step, base))
        base += full // step
    outs = pl.pallas_call(
        functools.partial(scale_kernel, tuple(plan)),
        out_shape=[jax.ShapeDtypeStruct((full, w), bf16) for w in widths]
        + [jax.ShapeDtypeStruct((1, w), f32) for w in widths]
        + [jax.ShapeDtypeStruct(norm_shape, bf16)],
        in_specs=[pl.BlockSpec(memory_space=pltpu.VMEM)] * 7,
        out_specs=[hbm] * 3 + [vmem] * 4,
        scratch_shapes=[pltpu.VMEM((full, w), bf16) for w in widths] + [dma((base,))],
        compiler_params=pltpu.CompilerParams(vmem_limit_bytes=18 * MIB),
        cost_estimate=pl.CostEstimate(flops=0, bytes_accessed=40 * MIB, transcendentals=0),
        name="scale",
    )(*(pltpu.with_memory_space_constraint(x, pltpu.VMEM) for x in parts))
    return (*outs[:3], *(o.reshape(-1) for o in outs[3:]))


def solution(mesh):
    in_specs = (
        P(("unit", "shard"), "model"),
        P(("unit", "shard"), None),
        P("unit", "model"),
        P(("unit", "shard"), "model"),
        P(("unit", "shard"), None),
        P("unit", "model"),
        P(("unit", "shard"), "model"),
        P(("unit", "shard"), None),
        P("unit", "model"),
        P(("unit", "shard", "model")),
        P(("unit", "shard", "model")),
    )
    out_specs = (
        P("unit", "model"),
        P("unit", "model"),
        P("unit", "model"),
        P(("unit", "model")),
        P(("unit", "model")),
        P(("unit", "model")),
        P("unit"),
    )
    body = functools.partial(local, mesh.shape["shard"], mesh.shape["model"])
    return jax.shard_map(body, mesh=mesh, in_specs=in_specs, out_specs=out_specs, check_vma=False)
```

```python
import functools

import jax
import jax.numpy as jnp
from jax import lax
from jax.experimental import pallas as pl
from jax.experimental.pallas import tpu as pltpu
from jax.sharding import PartitionSpec as P

mix_rate = 1.0
MESH = pl.DeviceIdType.MESH
MIB = 1 << 20


def exchange_kernel(
    n_shard,
    n_model,
    tile,
    tq, lq, hq, tk, lk, hk, tv, lv, hv, nt, ns,
    wq, wk, wv, sq, sk, sv, norm,
    base_q, base_k, base_v, low_q, low_k, low_v, high_q, high_k, high_v, norms,
    send_base, recv_base, send_low, recv_low, local_high, send_norm, recv_norm,
):
    trains, lows, highs = (tq, tk, tv), (lq, lk, lv), (hq, hk, hv)
    bases, low_bufs, high_bufs = (base_q, base_k, base_v), (low_q, low_k, low_v), (high_q, high_k, high_v)
    wholes, scales = (wq, wk, wv), (sq, sk, sv)
    rows = tq.shape[0]
    steps = rows // tile
    shard, model = lax.axis_index("shard"), lax.axis_index("model")
    group = n_shard * n_model
    place = shard * n_model + model

    barrier = pltpu.get_barrier_semaphore()
    for k in range(1, group):
        other = lax.rem(place + k, group)
        pl.semaphore_signal(
            barrier, inc=1,
            device_id={"shard": other // n_model, "model": lax.rem(other, n_model)},
            device_id_type=MESH,
        )

    def own_base(t, i):
        at = pl.ds(t * tile, tile)
        return pltpu.make_async_copy(trains[i].at[at, :], bases[i].at[0, at, :], recv_base.at[0, t, i])

    local = []
    for i in range(3):
        local.append(pltpu.make_async_copy(lows[i], low_bufs[i].at[0], recv_low.at[0, i]))
        local.append(pltpu.make_async_copy(highs[i], high_bufs[i], local_high.at[i]))
    for copy in local:
        copy.start()
    for t in range(steps):
        for i in range(3):
            own_base(t, i).start()
    own_norm = [
        pltpu.make_async_copy(source, norms.at[place, j], recv_norm.at[0, j])
        for j, source in enumerate((nt, ns))
    ]
    for copy in own_norm:
        copy.start()
    pl.semaphore_wait(barrier, group - 1)

    def low_copy(d, i):
        return pltpu.make_async_remote_copy(
            src_ref=lows[i], dst_ref=low_bufs[i].at[d],
            send_sem=send_low.at[d, i], recv_sem=recv_low.at[d, i],
            device_id={"shard": lax.rem(shard + d, n_shard)}, device_id_type=MESH,
        )

    def base_copy(d, t, i):
        at = pl.ds(t * tile, tile)
        return pltpu.make_async_remote_copy(
            src_ref=trains[i].at[at, :], dst_ref=bases[i].at[d, at, :],
            send_sem=send_base.at[d, t, i], recv_sem=recv_base.at[d, t, i],
            device_id={"shard": lax.rem(shard + d, n_shard)}, device_id_type=MESH,
        )

    def norm_copy(k, j):
        other = lax.rem(place + k, group)
        return pltpu.make_async_remote_copy(
            src_ref=(nt, ns)[j], dst_ref=norms.at[place, j],
            send_sem=send_norm.at[k, j], recv_sem=recv_norm.at[k, j],
            device_id={"shard": other // n_model, "model": lax.rem(other, n_model)},
            device_id_type=MESH,
        )

    for d in range(1, n_shard):
        for i in range(3):
            low_copy(d, i).start()
    for t in range(steps):
        for d in range(1, n_shard):
            for i in range(3):
                base_copy(d, t, i).start()
    for k in range(1, group):
        for j in range(2):
            norm_copy(k, j).start()

    def merge(d, t, tops):
        first = lax.rem(shard - d + n_shard, n_shard) * rows
        at = pl.multiple_of(t * tile, tile)
        to = pl.multiple_of(first + at, tile)
        new = []
        for i in range(3):
            top = tops[i]
            product = lax.dot_general(
                low_bufs[i][d, :, pl.ds(at, tile)], high_bufs[i][...],
                (((0,), (0,)), ((), ())), preferred_element_type=jnp.float32,
            )
            whole = bases[i][d, pl.ds(at, tile), :].astype(jnp.float32) + mix_rate * product
            wholes[i][pl.ds(to, tile), :] = whole
            top = jnp.maximum(top, jnp.max(jnp.abs(whole).reshape(tile // 8, 8, whole.shape[1]), axis=0))
            new.append(top)
        return tuple(new)

    tops = tuple(jnp.zeros((8, h.shape[1]), jnp.float32) for h in high_bufs)
    for copy in local:
        copy.wait()

    def own_step(t, tops):
        for i in range(3):
            own_base(t, i).wait()
        return merge(0, t, tops)

    tops = lax.fori_loop(0, steps, own_step, tops)
    for d in range(1, n_shard):
        for i in range(3):
            low_copy(d, i).wait()

    def other_step(u, tops):
        t, d = u // (n_shard - 1), 1 + lax.rem(u, n_shard - 1)
        for i in range(3):
            base_copy(d, t, i).wait()
        return merge(d, t, tops)

    tops = lax.fori_loop(0, steps * (n_shard - 1), other_step, tops)
    for i in range(3):
        scales[i][...] = jnp.max(tops[i], axis=0, keepdims=True)
    for copy in own_norm:
        copy.wait()
    for k in range(1, group):
        for j in range(2):
            norm_copy(k, j).wait()
    norm[...] = (norms[:, 0] + norms[:, 1]).reshape(norm.shape).astype(norm.dtype)


def scale_kernel(
    plan,
    wq, wk, wv, sq, sk, sv, norm,
    oq, ok, ov, osq, osk, osv, onorm,
    buf_q, buf_k, buf_v, sems, small_sems,
):
    wholes, scales = (wq, wk, wv), (sq, sk, sv)
    outs, bufs = (oq, ok, ov), (buf_q, buf_k, buf_v)
    small = [
        pltpu.make_async_copy(source, target, small_sems.at[n])
        for n, (source, target) in enumerate(((sq, osq), (sk, osk), (sv, osv), (norm, onorm)))
    ]
    for copy in small:
        copy.start()
    for i, step, count, base in plan:
        inverse = 1.0 / scales[i][...]

        def copy(t):
            at = pl.multiple_of(t * step, step)
            return pltpu.make_async_copy(
                bufs[i].at[pl.ds(at, step), :], outs[i].at[pl.ds(at, step), :], sems.at[base + t]
            )

        @pl.loop(0, count)
        def _(t):
            at = pl.multiple_of(t * step, step)
            bufs[i][pl.ds(at, step), :] = (wholes[i][pl.ds(at, step), :] * inverse).astype(bufs[i].dtype)
            copy(t).start()

    for i, step, count, base in plan:
        @pl.loop(0, count)
        def _(t):
            at = pl.multiple_of(t * step, step)
            pltpu.make_async_copy(
                bufs[i].at[pl.ds(at, step), :], outs[i].at[pl.ds(at, step), :], sems.at[base + t]
            ).wait()
    for copy in small:
        copy.wait()


def local(n_shard, n_model, tq, lq, hq, tk, lk, hk, tv, lv, hv, nt, ns):
    rows, rank = tq.shape[0], hq.shape[0]
    widths = (tq.shape[1], tk.shape[1], tv.shape[1])
    tile = min(rows, 256)
    steps = rows // tile
    group = n_shard * n_model
    lanes = 128 if nt.shape[0] % 128 == 0 else nt.shape[0]
    piece = (nt.shape[0] // lanes, lanes)
    full = n_shard * rows
    f32, bf16 = jnp.float32, jnp.bfloat16
    dma = pltpu.SemaphoreType.DMA
    hbm, vmem = pl.BlockSpec(memory_space=pltpu.HBM), pl.BlockSpec(memory_space=pltpu.VMEM)
    norm_shape = (group * piece[0], lanes)

    parts = pl.pallas_call(
        functools.partial(exchange_kernel, n_shard, n_model, tile),
        out_shape=[pltpu.VMEM((full, w), f32) for w in widths]
        + [pltpu.VMEM((1, w), f32) for w in widths]
        + [pltpu.VMEM(norm_shape, bf16)],
        in_specs=[hbm] * 11,
        out_specs=[vmem] * 7,
        scratch_shapes=[pltpu.VMEM((n_shard, rows, w), bf16) for w in widths]
        + [pltpu.VMEM((n_shard, rank, rows), bf16)] * 3
        + [pltpu.VMEM((rank, w), bf16) for w in widths]
        + [
            pltpu.VMEM((group, 2) + piece, f32),
            dma((n_shard, steps, 3)), dma((n_shard, steps, 3)),
            dma((n_shard, 3)), dma((n_shard, 3)), dma((3,)),
            dma((group, 2)), dma((group, 2)),
        ],
        compiler_params=pltpu.CompilerParams(
            collective_id=0, has_side_effects=True, vmem_limit_bytes=18 * MIB
        ),
        cost_estimate=pl.CostEstimate(flops=0, bytes_accessed=40 * MIB, transcendentals=0),
        name="exchange",
    )(*(pltpu.with_memory_space_constraint(x, pltpu.HBM) for x in (tq, lq.T, hq, tk, lk.T, hk, tv, lv.T, hv, nt.reshape(piece), ns.reshape(piece))))

    plan, base = [], 0
    for i in (0, 1, 2):
        step = min(full, 256 * max(widths) // widths[i])
        plan.append((i, step, full // step, base))
        base += full // step
    outs = pl.pallas_call(
        functools.partial(scale_kernel, tuple(plan)),
        out_shape=[jax.ShapeDtypeStruct((full, w), bf16) for w in widths]
        + [jax.ShapeDtypeStruct((1, w), f32) for w in widths]
        + [jax.ShapeDtypeStruct(norm_shape, bf16)],
        in_specs=[pl.BlockSpec(memory_space=pltpu.VMEM)] * 7,
        out_specs=[hbm] * 7,
        scratch_shapes=[pltpu.VMEM((full, w), bf16) for w in widths] + [dma((base,)), dma((4,))],
        compiler_params=pltpu.CompilerParams(vmem_limit_bytes=18 * MIB),
        cost_estimate=pl.CostEstimate(flops=0, bytes_accessed=40 * MIB, transcendentals=0),
        name="scale",
    )(*(pltpu.with_memory_space_constraint(x, pltpu.VMEM) for x in parts))
    return (*outs[:3], *(o.reshape(-1) for o in outs[3:]))


def solution(mesh):
    in_specs = (
        P(("unit", "shard"), "model"),
        P(("unit", "shard"), None),
        P("unit", "model"),
        P(("unit", "shard"), "model"),
        P(("unit", "shard"), None),
        P("unit", "model"),
        P(("unit", "shard"), "model"),
        P(("unit", "shard"), None),
        P("unit", "model"),
        P(("unit", "shard", "model")),
        P(("unit", "shard", "model")),
    )
    out_specs = (
        P("unit", "model"),
        P("unit", "model"),
        P("unit", "model"),
        P(("unit", "model")),
        P(("unit", "model")),
        P(("unit", "model")),
        P("unit"),
    )
    body = functools.partial(local, mesh.shape["shard"], mesh.shape["model"])
    return jax.shard_map(body, mesh=mesh, in_specs=in_specs, out_specs=out_specs, check_vma=False)
```
